32 devices in a mesh: blk: 8 (over y, x, core), ulysses: 4 (over z).
Axes of the slice: x: 2, y: 2, z: 4, core: 2. Of those that a mesh axis runs over, the one named last changes fastest.
Arguments:
- tokens: bfloat16 [2048, 3072], P(('blk', 'ulysses')), may hold values from -6 to 6
- mod_shift: float32 [3072], replicated, may hold values from -3 to 3
- mod_scale: float32 [3072], replicated, may hold values from -3 to 3
- mod_gate: float32 [3072], replicated, may hold values from 0.5 to 1.5
- qkv_weight: bfloat16 [3, 3072, 3072], P(None, None, 'ulysses'), may hold values from -0.109375 to 0.109375
- query_gain: float32 [128], replicated, may hold values from 1 to 16
- key_gain: float32 [128], replicated, may hold values from 1 to 16
- out_weight: bfloat16 [3072, 3072], P(None, 'ulysses'), may hold values from -0.109375 to 0.109375
Outputs:
- mixed: bfloat16 [2048, 3072], P(('blk', 'ulysses'))
The draws below stay inside these ranges and needn't reach their ends.
All inputs are finite; a program needn't handle non-finite values.
Results may differ from the reference program's by a relative error of at most 0.013.
The reference program's roundings to bfloat16 on the way (of `modulated`, `queries`, `keys`, `values`, `powers` and `attended`) count: a program that leaves them out, or rounds other values in their place, can miss the bound.
Values may be sent and summed in bfloat16 or wider, within the bound.
No kernel may reach another device: no remote copies, remote signals or barrier semaphores. Data moves between devices by JAX's collectives and lax.ppermute only.
A program may use at most 128 MiB of HBM per device.

```python
import math
import jax
import jax.numpy as jnp
from jax import lax

D = 3072
HEADS = 24
HEAD_DIM = 128
SEQ = 2048


def gain_vector(key, salt):
    base = jnp.exp(jax.random.uniform(jax.random.fold_in(key, salt), (HEAD_DIM,), jnp.float32, 0.0, 1.1))
    return base


def draw_query_gain(key, part):
    return gain_vector(key, 1)


def draw_key_gain(key, part):
    return gain_vector(key, 2)


def block_levels(stream_key, shape, shards, smallest, high):
    factor_of = 1.0
    for dim, blocks in shards:
        heights = jax.random.uniform(jax.random.fold_in(jax.random.fold_in(stream_key, 6), dim), (blocks,), jnp.float32, smallest / len(shards), high / len(shards))
        factor_of = factor_of * jnp.repeat(jnp.exp(heights), shape[dim] // blocks).reshape((-1,) + (1,) * (len(shape) - 1 - dim))
    return factor_of


def bell_draw(stream_key, shape, width, bound, cuts=(), held_as=jnp.bfloat16):
    loudness = block_levels(stream_key, shape, cuts, -0.22, 0.18) if cuts else 1.0
    values = jax.random.normal(stream_key, shape, jnp.float32) * width * loudness
    return jnp.minimum(jnp.maximum(values, -bound), bound).astype(held_as)


def setup_inputs(seed: int = 0) -> dict:
    streams_of = jax.random.split(jax.random.key(seed), 9)
    return {
        "tokens": bell_draw(streams_of[0], (SEQ, D), 1.0, 6.0, ((0, 32),)),
        "mod_shift": bell_draw(streams_of[1], (D,), 0.5, 3.0, (), jnp.float32),
        "mod_scale": bell_draw(streams_of[2], (D,), 0.5, 3.0, (), jnp.float32),
        "mod_gate": jnp.clip(jax.random.uniform(streams_of[3], (D,), jnp.float32, 0.5, 1.5), 0.5, 1.5),
        "qkv_weight": bell_draw(streams_of[4], (3, D, HEADS * HEAD_DIM), D ** -0.5, 0.109375, ((2, 4),)),
        "query_gain": draw_query_gain(jax.random.fold_in(streams_of[8], 71), 0),
        "key_gain": draw_key_gain(jax.random.fold_in(streams_of[8], 71), 0),
        "out_weight": bell_draw(streams_of[7], (HEADS * HEAD_DIM, D), (HEADS * HEAD_DIM) ** -0.5, 0.109375, ((1, 4),)),
    }


def head_norm(projected, gain, factor):
    split = projected.reshape(projected.shape[0], -1, gain.shape[0])
    meansq = lax.optimization_barrier(jnp.mean(split * split, axis=-1, keepdims=True))
    return (split * lax.rsqrt(meansq + 1e-06) * gain * factor).reshape(projected.shape)

def reference(tokens, mod_shift, mod_scale, mod_gate, qkv_weight, query_gain, key_gain, out_weight):
    wide = tokens.astype(jnp.float32)
    center = lax.optimization_barrier(jnp.mean(wide, axis=-1, keepdims=True))
    spread = lax.optimization_barrier(jnp.mean((wide - center) ** 2, axis=-1, keepdims=True))
    normed = (wide - center) / jnp.sqrt(spread + 1e-06)
    modulated = (normed * (1.0 + mod_scale) + mod_shift).astype(jnp.bfloat16)
    query_sums = jnp.dot(modulated, qkv_weight[0], preferred_element_type=jnp.float32)
    key_sums = jnp.dot(modulated, qkv_weight[1], preferred_element_type=jnp.float32)
    value_sums = jnp.dot(modulated, qkv_weight[2], preferred_element_type=jnp.float32)
    queries = head_norm(query_sums, query_gain, 1.0 / math.sqrt(HEAD_DIM)).astype(jnp.bfloat16)
    keys = head_norm(key_sums, key_gain, 1.0).astype(jnp.bfloat16)
    values = value_sums.astype(jnp.bfloat16)
    length = tokens.shape[0]
    block = math.gcd(length, 1024)

    def heads_first(matrix):
        return matrix.reshape(length, HEADS, HEAD_DIM).transpose(1, 0, 2)

    def one_head(operands):
        query_head, key_head, value_head = operands

        def one_block(query_block):
            scores = jnp.dot(query_block, key_head.T, preferred_element_type=jnp.float32)
            highest = lax.optimization_barrier(jnp.max(scores, axis=-1, keepdims=True))
            powers = jnp.exp(scores - highest)
            numerator = jnp.dot(powers.astype(jnp.bfloat16), value_head, preferred_element_type=jnp.float32)
            return numerator / lax.optimization_barrier(jnp.sum(powers, axis=-1, keepdims=True))
        result = lax.map(one_block, query_head.reshape(length // block, block, HEAD_DIM))
        return result.reshape(length, HEAD_DIM)
    attended = lax.map(one_head, (heads_first(queries), heads_first(keys), heads_first(values)))
    attended = attended.transpose(1, 0, 2).reshape(length, HEADS * HEAD_DIM).astype(jnp.bfloat16)
    branch = jnp.dot(attended, out_weight, preferred_element_type=jnp.float32)
    return (wide + mod_gate * branch).astype(jnp.bfloat16)
```

```python
import functools
import math

import jax
import jax.numpy as jnp
from jax import lax
from jax.experimental import pallas as pl
from jax.experimental.pallas import tpu as pltpu
from jax.sharding import PartitionSpec as P


F32 = jnp.float32
BF16 = jnp.bfloat16


def norm_kernel(tokens_ref, shift_ref, scale_ref, out_ref):
    wide = tokens_ref[...].astype(F32)
    center = jnp.mean(wide, axis=-1, keepdims=True)
    spread = jnp.mean((wide - center) ** 2, axis=-1, keepdims=True)
    normed = (wide - center) / jnp.sqrt(spread + 1e-06)
    out_ref[...] = (normed * (1.0 + scale_ref[...]) + shift_ref[...]).astype(BF16)


def modulate(tokens, shift, scale):
    return pl.pallas_call(
        norm_kernel,
        out_shape=jax.ShapeDtypeStruct(tokens.shape, BF16),
        name="modulate",
    )(tokens, shift[None], scale[None])


def chain_gather(block, axis, count):
    place = lax.axis_index(axis)
    from_left = [block]
    from_right = [block]
    for hop in range(1, count):
        up = [(i, i + 1) for i in range(hop - 1, count - 1)]
        down = [(count - 1 - a, count - 1 - b) for a, b in up]
        from_left.append(lax.ppermute(from_left[-1], axis, up))
        from_right.append(lax.ppermute(from_right[-1], axis, down))
    ordered = []
    for source in range(count):
        piece = block
        for hop in range(1, count):
            if source + hop < count:
                piece = jnp.where(place == source + hop, from_left[hop], piece)
            if source - hop >= 0:
                piece = jnp.where(place == source - hop, from_right[hop], piece)
        ordered.append(piece)
    return ordered


def project_kernel(first, splits, head, factors, core_ref, rows_ref, weight_ref, gains_ref, *out_refs):
    job = pl.program_id(0)
    sums = jnp.dot(rows_ref[...], weight_ref[0], preferred_element_type=F32)
    width = sums.shape[1]
    each = width // splits

    def store(results):
        joined = [
            jnp.concatenate(results[s * each // head : (s + 1) * each // head], axis=1)
            for s in range(splits)
        ]
        if splits == 1:
            out_refs[0][0] = joined[0]
        else:
            @pl.when(core_ref[0] == 0)
            def _():
                out_refs[0][0] = joined[0]
                out_refs[1][0] = joined[1]

            @pl.when(core_ref[0] != 0)
            def _():
                out_refs[0][0] = joined[1]
                out_refs[1][0] = joined[0]

    pieces = [sums[:, h * head : (h + 1) * head] for h in range(width // head)]

    def normed(which):
        gain = gains_ref[which : which + 1]
        out = []
        for piece in pieces:
            meansq = jnp.mean(piece * piece, axis=-1, keepdims=True)
            out.append((piece * lax.rsqrt(meansq + 1e-06) * gain * factors[which]).astype(BF16))
        return out

    if first == 0:
        store(normed(0))
    else:
        @pl.when(job == 0)
        def _():
            store(normed(1))

        @pl.when(job == 1)
        def _():
            store([piece.astype(BF16) for piece in pieces])


def project(core, rows, weight, gains, first, jobs, splits, factors):
    count, depth = rows.shape
    width = weight.shape[2]
    head = gains.shape[1]
    each = width // splits
    return pl.pallas_call(
        functools.partial(project_kernel, first, splits, head, factors),
        grid_spec=pltpu.PrefetchScalarGridSpec(
            num_scalar_prefetch=1,
            grid=(jobs,),
            in_specs=[
                pl.BlockSpec((count, depth), lambda j, c: (0, 0)),
                pl.BlockSpec((1, depth, width), lambda j, c: (j + first, 0, 0)),
                pl.BlockSpec(gains.shape, lambda j, c: (0, 0)),
            ],
            out_specs=[pl.BlockSpec((1, count, each), lambda j, c: (j, 0, 0))] * splits,
        ),
        out_shape=[jax.ShapeDtypeStruct((jobs, count, each), BF16)] * splits,
        name=f"project{first}",
    )(core, rows, weight, gains)


def attend_kernel(parts, query_ref, *refs):
    keys, values, out_ref = refs[:parts], refs[parts : 2 * parts], refs[2 * parts]
    query = query_ref[...]
    scores = [
        lax.dot_general(query, k[...], (((1,), (1,)), ((), ())), preferred_element_type=F32)
        for k in keys
    ]
    highest = functools.reduce(
        jnp.maximum, [jnp.max(s, axis=-1, keepdims=True) for s in scores]
    )
    total = 0.0
    numerator = 0.0
    for s, v in zip(scores, values):
        powers = jnp.exp(s - highest)
        total = total + jnp.sum(powers, axis=-1, keepdims=True)
        numerator = numerator + jnp.dot(powers.astype(BF16), v[...], preferred_element_type=F32)
    out_ref[...] = (numerator / total).astype(BF16)


def attend(query, keys, values, head, tile):
    rows, width = query.shape
    parts = len(keys)
    key_specs = [pl.BlockSpec((k.shape[0], head), lambda h, t: (0, h)) for k in keys]
    return pl.pallas_call(
        functools.partial(attend_kernel, parts),
        grid=(width // head, rows // tile),
        in_specs=[pl.BlockSpec((tile, head), lambda h, t: (t, h))] + key_specs + key_specs,
        out_specs=pl.BlockSpec((tile, head), lambda h, t: (t, h)),
        out_shape=jax.ShapeDtypeStruct((rows, width), BF16),
        name="attend",
    )(query, *keys, *values)


def local(blocks, group, tokens, mod_shift, mod_scale, mod_gate, qkv_weight, query_gain, key_gain, out_weight):
    head = query_gain.shape[0]
    heads_here = qkv_weight.shape[2] // head
    factors = (1.0 / math.sqrt(head), 1.0)
    gains = jnp.stack([query_gain, key_gain])
    modulated = modulate(tokens, mod_shift, mod_scale)
    rows = jnp.concatenate(chain_gather(modulated, "ulysses", group), axis=0)
    own = rows.shape[0]
    core = lax.axis_index("blk") % 2
    core_list = core.astype(jnp.int32)[None]

    def across(array, mask):
        return lax.ppermute(array, "blk", [(i, i ^ mask) for i in range(blocks)])

    paired = heads_here % 2 == 0 and blocks == 8
    splits = 2 if paired else 1
    kv = project(core_list, rows, qkv_weight, gains, 1, 2, splits, factors)
    q = project(core_list, rows, qkv_weight, gains, 0, 1, splits, factors)
    tile = math.gcd(own, 256)
    if paired:
        kv_other = across(kv[1], 1)
        q_other = across(q[1], 1)
        key = jnp.concatenate([kv[0][0], kv_other[0]], axis=0)
        value = jnp.concatenate([kv[0][1], kv_other[1]], axis=0)
        query = jnp.concatenate([q[0][0], q_other[0]], axis=0)
        key_x = across(key, 2)
        value_y = across(value, 4)
        value_x = across(value, 2)
        key_y = across(key, 4)
        key_d = across(key_x, 4)
        value_d = across(value_y, 2)
        out = attend(query, [key, key_x, key_y, key_d], [value, value_x, value_y, value_d], head, tile)
        mine = out[:own]
        theirs = across(out[own:], 1)
        attended = jnp.concatenate(
            [jnp.where(core == 0, mine, theirs), jnp.where(core == 0, theirs, mine)], axis=1
        )
    else:
        key = lax.all_gather(kv[0][0], "blk", axis=0, tiled=True)
        value = lax.all_gather(kv[0][1], "blk", axis=0, tiled=True)
        attended = attend(q[0][0], [key], [value], head, math.gcd(own, 128))
    everything = jnp.concatenate(chain_gather(attended, "ulysses", group), axis=1)
    columns = jnp.dot(everything, out_weight, preferred_element_type=F32)
    branch = lax.all_to_all(
        columns.astype(BF16), "ulysses", split_axis=0, concat_axis=1, tiled=True
    ).astype(F32)
    return (tokens.astype(F32) + mod_gate * branch).astype(BF16)


def solution(mesh):
    in_specs = (
        P(("blk", "ulysses"), None),
        P(),
        P(),
        P(),
        P(None, None, "ulysses"),
        P(),
        P(),
        P(None, "ulysses"),
    )
    out_specs = P(("blk", "ulysses"), None)
    body = functools.partial(local, mesh.shape["blk"], mesh.shape["ulysses"])
    return jax.shard_map(body, mesh=mesh, in_specs=in_specs, out_specs=out_specs, check_vma=False)
```

```python
import functools
import math

import jax
import jax.numpy as jnp
from jax import lax
from jax.experimental import pallas as pl
from jax.experimental.pallas import tpu as pltpu
from jax.sharding import PartitionSpec as P


F32 = jnp.float32
BF16 = jnp.bfloat16
PARTS = 2


def norm_kernel(tokens_ref, shift_ref, scale_ref, *out_refs):
    rows = out_refs[0].shape[0]
    for part, out_ref in enumerate(out_refs):
        wide = tokens_ref[part * rows : (part + 1) * rows].astype(F32)
        center = jnp.mean(wide, axis=-1, keepdims=True)
        spread = jnp.mean((wide - center) ** 2, axis=-1, keepdims=True)
        normed = (wide - center) / jnp.sqrt(spread + 1e-06)
        out_ref[...] = (normed * (1.0 + scale_ref[...]) + shift_ref[...]).astype(BF16)


def modulate(tokens, shift, scale):
    shape = (tokens.shape[0] // PARTS, tokens.shape[1])
    return pl.pallas_call(
        norm_kernel,
        out_shape=[jax.ShapeDtypeStruct(shape, BF16)] * PARTS,
        name="modulate",
    )(tokens, shift[None], scale[None])


def chains(block, axis, count):
    found = {0: block}
    for hop in range(1, count):
        up = [(i, i + 1) for i in range(hop - 1, count - 1)]
        down = [(count - 1 - a, count - 1 - b) for a, b in up]
        found[hop] = lax.ppermute(found[hop - 1], axis, up)
        found[-hop] = lax.ppermute(found[1 - hop], axis, down)
    return found


def order_kernel(count, place_ref, *refs):
    sources = {d: refs[d + count - 1] for d in range(1 - count, count)}
    out_ref, sems = refs[2 * count - 1 :]
    rows = sources[0].shape[0]
    for place in range(count):

        @pl.when(place_ref[0] == place)
        def _(place=place):
            copies = [
                pltpu.make_async_copy(
                    sources[place - s], out_ref.at[pl.ds(s * rows, rows)], sems.at[s]
                )
                for s in range(count)
            ]
            for copy in copies:
                copy.start()
            for copy in copies:
                copy.wait()


def in_order(place, found, count):
    rows, width = found[0].shape
    blocks = [found[d] for d in range(1 - count, count)]
    return pl.pallas_call(
        functools.partial(order_kernel, count),
        in_specs=[pl.BlockSpec(memory_space=pltpu.SMEM)]
        + [pl.BlockSpec(memory_space=pl.ANY)] * len(blocks),
        out_shape=jax.ShapeDtypeStruct((rows * count, width), BF16),
        scratch_shapes=[pltpu.SemaphoreType.DMA((count,))],
        name="in_order",
    )(place, *blocks)


def project_kernel(first, head, factors, core_ref, rows_ref, other_ref, weight_ref, gains_ref, out_ref):
    rows = jnp.concatenate([rows_ref[...], other_ref[...]], axis=0)
    sums = jnp.dot(rows, weight_ref[0], preferred_element_type=F32)

    def normed(which):
        gain = gains_ref[which : which + 1]
        for h in range(sums.shape[1] // head):
            piece = sums[:, h * head : (h + 1) * head]
            meansq = jnp.mean(piece * piece, axis=-1, keepdims=True)
            piece = piece * lax.rsqrt(meansq + 1e-06) * gain * factors[which]
            out_ref[0, :, h * head : (h + 1) * head] = piece.astype(BF16)

    if first == 0:
        normed(0)
    else:
        job = pl.program_id(0)

        @pl.when(job == 0)
        def _():
            normed(1)

        @pl.when(job == 1)
        def _():
            out_ref[0] = sums.astype(BF16)


def project(core, rows, other, weight, gains, first, jobs, factors):
    count, depth = rows.shape
    width = weight.shape[2] // 2
    return pl.pallas_call(
        functools.partial(project_kernel, first, gains.shape[1], factors),
        grid_spec=pltpu.PrefetchScalarGridSpec(
            num_scalar_prefetch=1,
            grid=(jobs,),
            in_specs=[
                pl.BlockSpec((count, depth), lambda j, c: (0, 0)),
                pl.BlockSpec((count, depth), lambda j, c: (0, 0)),
                pl.BlockSpec((1, depth, width), lambda j, c: (j + first, 0, c[0])),
                pl.BlockSpec(gains.shape, lambda j, c: (0, 0)),
            ],
            out_specs=pl.BlockSpec((1, 2 * count, width), lambda j, c: (j, 0, 0)),
        ),
        out_shape=jax.ShapeDtypeStruct((jobs, 2 * count, width), BF16),
        name=f"project{first}",
    )(core, rows, other, weight, gains)


def partial_softmax(query, pairs, state):
    scores = [
        lax.dot_general(query, kv[0], (((1,), (1,)), ((), ())), preferred_element_type=F32)
        for kv in pairs
    ]
    highest = functools.reduce(jnp.maximum, [jnp.max(s, axis=-1, keepdims=True) for s in scores])
    total = 0.0
    numerator = 0.0
    if state is not None:
        numerator, before, total = state
        highest = jnp.maximum(highest, before)
        rescale = jnp.exp(before - highest)
        total = total * rescale
        numerator = numerator * rescale
    for s, kv in zip(scores, pairs):
        powers = jnp.exp(s - highest)
        total = total + jnp.sum(powers, axis=-1, keepdims=True)
        numerator = numerator + jnp.dot(powers.astype(BF16), kv[1], preferred_element_type=F32)
    return numerator, highest, total


def begin_kernel(parts, *refs):
    pairs = refs[PARTS : PARTS + parts]
    outs = refs[PARTS + parts :]
    for part in range(PARTS):
        result = partial_softmax(refs[part][0], pairs, None)
        for out_ref, array in zip(outs[3 * part : 3 * part + 3], result):
            out_ref[...] = jnp.broadcast_to(array, out_ref.shape)


def begin(queries, pairs, head):
    _, rows, width = queries[0].shape
    whole = [pl.BlockSpec((a.shape[0], a.shape[1], head), lambda h: (0, 0, h)) for a in (*queries, *pairs)]
    return pl.pallas_call(
        functools.partial(begin_kernel, len(pairs)),
        grid=(width // head,),
        in_specs=whole,
        out_specs=[pl.BlockSpec((rows, head), lambda h: (0, h))] * (3 * PARTS),
        out_shape=[jax.ShapeDtypeStruct((rows, width), F32)] * (3 * PARTS),
        name="attend_begin",
    )(*queries, *pairs)


def finish_kernel(parts, query_ref, numerator_ref, highest_ref, total_ref, *refs):
    mine_ref, other_ref = refs[parts:]
    state = (numerator_ref[...], highest_ref[:, :1], total_ref[:, :1])
    numerator, _, total = partial_softmax(query_ref[0], refs[:parts], state)
    out = (numerator / total).astype(BF16)
    half = out.shape[0] // 2
    mine_ref[...] = out[:half]
    other_ref[...] = out[half:]


def finish(query, state, pairs, head):
    _, rows, width = query.shape
    spec = pl.BlockSpec((rows, head), lambda h: (0, h))
    whole = [pl.BlockSpec((a.shape[0], a.shape[1], head), lambda h: (0, 0, h)) for a in (query, *pairs)]
    return pl.pallas_call(
        functools.partial(finish_kernel, len(pairs)),
        grid=(width // head,),
        in_specs=[whole[0]] + [spec] * 3 + whole[1:],
        out_specs=[pl.BlockSpec((rows // 2, head), lambda h: (0, h))] * 2,
        out_shape=[jax.ShapeDtypeStruct((rows // 2, width), BF16)] * 2,
        name="attend_finish",
    )(query, *state, *pairs)


def mix_kernel(count, place_ref, *refs):
    sources = {d: refs[d + count - 1] for d in range(1 - count, count)}
    weight_ref = refs[2 * count - 1]
    outs = refs[2 * count : 3 * count]
    block_ref, sums_ref = refs[3 * count :]
    step = pl.program_id(0)
    place = place_ref[0]
    for d in range(1 - count, count):

        @pl.when(place - step == d)
        def _(d=d):
            block_ref[...] = sources[d][...]

    sums = jnp.dot(block_ref[...], weight_ref[...], preferred_element_type=F32)

    @pl.when(step == 0)
    def _():
        sums_ref[...] = sums

    @pl.when(step != 0)
    def _():
        sums_ref[...] += sums

    @pl.when(step == count - 1)
    def _():
        rows = outs[0].shape[0]
        for d in range(count):
            owner = lax.rem(place + d, count)
            outs[d][...] = sums_ref[pl.ds(pl.multiple_of(owner * rows, rows), rows)].astype(BF16)


def mix(place, found, weight, count):
    rows, width = found[0].shape
    columns = weight.shape[1]
    blocks = [found[d] for d in range(1 - count, count)]
    return pl.pallas_call(
        functools.partial(mix_kernel, count),
        grid_spec=pltpu.PrefetchScalarGridSpec(
            num_scalar_prefetch=1,
            grid=(count,),
            in_specs=[pl.BlockSpec((rows, width), lambda s, p: (0, 0))] * len(blocks)
            + [pl.BlockSpec((width, columns), lambda s, p: (s, 0))],
            out_specs=[pl.BlockSpec((rows // count, columns), lambda s, p: (0, 0))] * count,
            scratch_shapes=[pltpu.VMEM((rows, width), BF16), pltpu.VMEM((rows, columns), F32)],
        ),
        out_shape=[jax.ShapeDtypeStruct((rows // count, columns), BF16)] * count,
        name="mix",
    )(place, *blocks, weight)


def gate_kernel(count, place_ref, tokens_ref, gate_ref, *refs):
    out_ref = refs[-1]
    rows, columns = refs[0].shape
    for part in range(PARTS):
        span = slice(part * rows, (part + 1) * rows)
        for d in range(count):
            source = lax.rem(place_ref[0] - d + count, count)
            here = pl.ds(pl.multiple_of(source * columns, columns), columns)
            branch = refs[part * count + d][...].astype(F32)
            out_ref[span, here] = (
                tokens_ref[span, here].astype(F32) + gate_ref[:, here] * branch
            ).astype(BF16)


def gated(place, tokens, gate, branches, count):
    whole = pl.BlockSpec(memory_space=pltpu.VMEM)
    return pl.pallas_call(
        functools.partial(gate_kernel, count),
        in_specs=[pl.BlockSpec(memory_space=pltpu.SMEM)] + [whole] * (2 + len(branches)),
        out_specs=whole,
        out_shape=jax.ShapeDtypeStruct(tokens.shape, BF16),
        name="gated",
    )(place, tokens, gate[None], *branches)


def paired(blocks, group, tokens, mod_shift, mod_scale, mod_gate, qkv_weight, query_gain, key_gain, out_weight):
    head = query_gain.shape[0]
    factors = (1.0 / math.sqrt(head), 1.0)
    gains = jnp.stack([query_gain, key_gain])
    core = lax.axis_index("blk") % 2
    core_list = core.astype(jnp.int32)[None]
    place = lax.axis_index("ulysses").astype(jnp.int32)[None]

    def across(array, mask):
        return lax.ppermute(array, "blk", [(i, i ^ mask) for i in range(blocks)])

    parts = [chains(block, "ulysses", group) for block in modulate(tokens, mod_shift, mod_scale)]
    rows = [in_order(place, found, group) for found in parts]
    others = [across(r, 1) for r in rows]
    kv = [project(core_list, r, o, qkv_weight, gains, 1, 2, factors) for r, o in zip(rows, others)]
    q = [project(core_list, r, o, qkv_weight, gains, 0, 1, factors) for r, o in zip(rows, others)]
    along_x = [across(a, 2) for a in kv]
    along_y = [across(a, 4) for a in kv]
    far = [across(along_x[0], 4), across(along_y[1], 2)]
    states = begin(q, [kv[0], kv[1], along_x[0], along_y[0], far[0]], head)
    late = [along_x[1], along_y[1], far[1]]
    branches = []
    for part in range(PARTS):
        mine, send = finish(q[part], states[3 * part : 3 * part + 3], late, head)
        theirs = across(send, 1)
        attended = jnp.concatenate(
            [jnp.where(core == 0, mine, theirs), jnp.where(core == 0, theirs, mine)], axis=1
        )
        found = chains(attended, "ulysses", group)
        columns = mix(place, found, out_weight, group)
        branches.append(columns[0])
        for d in range(1, group):
            shift = [(i, (i + d) % group) for i in range(group)]
            branches.append(lax.ppermute(columns[d], "ulysses", shift))
    return gated(place, tokens, mod_gate, branches, group)


def head_norm(projected, gain, factor):
    split = projected.reshape(projected.shape[0], -1, gain.shape[0])
    meansq = jnp.mean(split * split, axis=-1, keepdims=True)
    return (split * lax.rsqrt(meansq + 1e-06) * gain * factor).reshape(projected.shape)


def local(tokens, mod_shift, mod_scale, mod_gate, qkv_weight, query_gain, key_gain, out_weight):
    wide = tokens.astype(jnp.float32)
    center = jnp.mean(wide, axis=-1, keepdims=True)
    spread = jnp.mean((wide - center) ** 2, axis=-1, keepdims=True)
    normed = (wide - center) / jnp.sqrt(spread + 1e-06)
    modulated = (normed * (1.0 + mod_scale) + mod_shift).astype(jnp.bfloat16)
    head_size = query_gain.shape[0]
    local_width = qkv_weight.shape[2]
    heads_here = local_width // head_size
    factor = 1.0 / math.sqrt(head_size)
    sums = jnp.einsum(
        "rd,jde->jre",
        lax.all_gather(modulated, "ulysses", axis=0, tiled=True),
        qkv_weight,
        preferred_element_type=jnp.float32,
    )
    queries = head_norm(sums[0], query_gain, factor)
    keys = head_norm(sums[1], key_gain, 1.0)
    stacked = jnp.stack([queries, keys, sums[2]]).astype(jnp.bfloat16)
    queries, keys, values = (stacked[0], stacked[1], stacked[2])
    query_rows = queries.shape[0]
    query_heads = queries.reshape(query_rows, heads_here, head_size)
    start_state = (
        jnp.full((heads_here, query_rows), -1e30, jnp.float32),
        jnp.zeros((heads_here, query_rows), jnp.float32),
        jnp.zeros((heads_here, query_rows, head_size), jnp.float32),
    )
    key_part = lax.all_gather(keys, "blk", axis=0, tiled=True)
    value_part = lax.all_gather(values, "blk", axis=0, tiled=True)
    count = key_part.shape[0] // query_rows

    def step(position, state):
        highest, total, numerator = state
        key_block = lax.dynamic_slice_in_dim(key_part, position * query_rows, query_rows, 0)
        value_block = lax.dynamic_slice_in_dim(value_part, position * query_rows, query_rows, 0)
        key_block = key_block.reshape(query_rows, heads_here, head_size)
        value_block = value_block.reshape(query_rows, heads_here, head_size)
        scores = jnp.einsum(
            "qhd,khd->hqk", query_heads, key_block, preferred_element_type=jnp.float32
        )
        new_high = jnp.maximum(highest, jnp.max(scores, axis=-1))
        rescale = jnp.exp(highest - new_high)
        powers = jnp.exp(scores - new_high[..., None])
        total = total * rescale + jnp.sum(powers, axis=-1)
        numerator = numerator * rescale[..., None] + jnp.einsum(
            "hqk,khd->hqd",
            powers.astype(jnp.bfloat16),
            value_block,
            preferred_element_type=jnp.float32,
        )
        return (new_high, total, numerator)

    highest, total, numerator = lax.fori_loop(0, count, step, start_state)
    attended = (numerator / total[..., None]).transpose(1, 0, 2).reshape(query_rows, local_width)
    attended = attended.astype(jnp.bfloat16)
    columns = jnp.dot(
        lax.all_gather(attended, "ulysses", axis=1, tiled=True),
        out_weight,
        preferred_element_type=jnp.float32,
    )
    branch = lax.all_to_all(
        columns.astype(jnp.bfloat16), "ulysses", split_axis=0, concat_axis=1, tiled=True
    ).astype(columns.dtype)
    return (wide + mod_gate * branch).astype(jnp.bfloat16)


def solution(mesh):
    in_specs = (
        P(("blk", "ulysses"), None),
        P(),
        P(),
        P(),
        P(None, None, "ulysses"),
        P(),
        P(),
        P(None, "ulysses"),
    )
    out_specs = P(("blk", "ulysses"), None)
    blocks, group = mesh.shape["blk"], mesh.shape["ulysses"]

    def body(*args):
        tokens, head, width = args[0], args[5].shape[0], args[4].shape[2]
        pairs_split = width % (2 * head) == 0 and tokens.shape[0] % (16 * PARTS) == 0
        if blocks == 8 and pairs_split:
            return paired(blocks, group, *args)
        return local(*args)

    return jax.shard_map(body, mesh=mesh, in_specs=in_specs, out_specs=out_specs, check_vma=False)
```

```python
import functools
import math

import jax
import jax.numpy as jnp
from jax import lax
from jax.experimental import pallas as pl
from jax.experimental.pallas import tpu as pltpu
from jax.sharding import PartitionSpec as P


F32 = jnp.float32
BF16 = jnp.bfloat16
PARTS = 2


def norm_kernel(tokens_ref, shift_ref, scale_ref, *out_refs):
    rows = out_refs[0].shape[0]
    for part, out_ref in enumerate(out_refs):
        wide = tokens_ref[part * rows : (part + 1) * rows].astype(F32)
        center = jnp.mean(wide, axis=-1, keepdims=True)
        spread = jnp.mean((wide - center) ** 2, axis=-1, keepdims=True)
        normed = (wide - center) / jnp.sqrt(spread + 1e-06)
        out_ref[...] = (normed * (1.0 + scale_ref[...]) + shift_ref[...]).astype(BF16)


def modulate(tokens, shift, scale):
    shape = (tokens.shape[0] // PARTS, tokens.shape[1])
    return pl.pallas_call(
        norm_kernel,
        out_shape=[jax.ShapeDtypeStruct(shape, BF16)] * PARTS,
        name="modulate",
    )(tokens, shift[None], scale[None])


def chains(block, axis, count):
    found = {0: block}
    for hop in range(1, count):
        up = [(i, i + 1) for i in range(hop - 1, count - 1)]
        down = [(count - 1 - a, count - 1 - b) for a, b in up]
        found[hop] = lax.ppermute(found[hop - 1], axis, up)
        found[-hop] = lax.ppermute(found[1 - hop], axis, down)
    return found


def project_kernel(count, head, factor, core_ref, place_ref, *refs):
    blocks = refs[: PARTS * (2 * count - 1)]
    weight_ref, gains_ref, keep_ref, send_ref, rows_ref = refs[len(blocks) :]
    job = pl.program_id(0)
    each = blocks[0].shape[0]

    @pl.when(job == 0)
    def _():
        for part in range(PARTS):
            for place in range(count):

                @pl.when(place_ref[0] == place)
                def _(part=part, place=place):
                    for s in range(count):
                        start = (part * count + s) * each
                        block = blocks[part * (2 * count - 1) + place - s + count - 1]
                        rows_ref[start : start + each] = block[...]

    sums = jnp.dot(rows_ref[...], weight_ref[0], preferred_element_type=F32)
    finish_projection(job, sums, head, factor, core_ref, gains_ref, keep_ref, send_ref)


def again_kernel(head, factor, core_ref, rows_ref, weight_ref, gains_ref, keep_ref, send_ref):
    sums = jnp.dot(rows_ref[...], weight_ref[0], preferred_element_type=F32)
    finish_projection(0, sums, head, factor, core_ref, gains_ref, keep_ref, send_ref)


def finish_projection(job, sums, head, factor, core_ref, gains_ref, keep_ref, send_ref):
    half = sums.shape[1] // 2
    heads = half // head

    def store(pieces):
        for core in range(2):

            @pl.when(core_ref[0] == core)
            def _(core=core):
                for out_ref, side in ((keep_ref, core), (send_ref, 1 - core)):
                    for h in range(heads):
                        out_ref[0, :, h * head : (h + 1) * head] = pieces[side * heads + h]

    pieces = [sums[:, h * head : (h + 1) * head] for h in range(2 * heads)]

    def normed():
        out = []
        for piece in pieces:
            meansq = jnp.mean(piece * piece, axis=-1, keepdims=True)
            out.append((piece * lax.rsqrt(meansq + 1e-06) * gains_ref[...] * factor).astype(BF16))
        return out

    if isinstance(job, int):
        store(normed())
    else:

        @pl.when(job == 0)
        def _():
            store(normed())

        @pl.when(job != 0)
        def _():
            store([piece.astype(BF16) for piece in pieces])


def project(core, place, parts, weight, gain, count):
    each, depth = parts[0][0].shape
    width = weight.shape[2]
    rows = PARTS * count * each
    blocks = [found[d] for found in parts for d in range(1 - count, count)]
    kept = pl.BlockSpec((1, rows, width // 2), lambda j, c, p: (j, 0, 0))
    return pl.pallas_call(
        functools.partial(project_kernel, count, gain.shape[0], 1.0),
        grid_spec=pltpu.PrefetchScalarGridSpec(
            num_scalar_prefetch=2,
            grid=(2,),
            in_specs=[pl.BlockSpec((each, depth), lambda j, c, p: (0, 0))] * len(blocks)
            + [
                pl.BlockSpec((1, depth, width), lambda j, c, p: (j + 1, 0, 0)),
                pl.BlockSpec((1, gain.shape[0]), lambda j, c, p: (0, 0)),
            ],
            out_specs=[kept, kept, pl.BlockSpec((rows, depth), lambda j, c, p: (0, 0))],
        ),
        out_shape=[jax.ShapeDtypeStruct((2, rows, width // 2), BF16)] * 2
        + [jax.ShapeDtypeStruct((rows, depth), BF16)],
        name="project_kv",
    )(core, place, *blocks, weight, gain[None])


def project_query(core, rows, weight, gain):
    count, depth = rows.shape
    width = weight.shape[2]
    kept = pl.BlockSpec((1, count, width // 2), lambda j, c: (0, 0, 0))
    return pl.pallas_call(
        functools.partial(again_kernel, gain.shape[0], 1.0 / math.sqrt(gain.shape[0])),
        grid_spec=pltpu.PrefetchScalarGridSpec(
            num_scalar_prefetch=1,
            grid=(1,),
            in_specs=[
                pl.BlockSpec((count, depth), lambda j, c: (0, 0)),
                pl.BlockSpec((1, depth, width), lambda j, c: (0, 0, 0)),
                pl.BlockSpec((1, gain.shape[0]), lambda j, c: (0, 0)),
            ],
            out_specs=[kept, kept],
        ),
        out_shape=[jax.ShapeDtypeStruct((1, count, width // 2), BF16)] * 2,
        name="project_q",
    )(core, rows, weight, gain[None])


def partial_softmax(query, pairs, state):
    scores = [
        lax.dot_general(query, kv[0], (((1,), (1,)), ((), ())), preferred_element_type=F32)
        for kv in pairs
    ]
    highest = functools.reduce(jnp.maximum, [jnp.max(s, axis=-1, keepdims=True) for s in scores])
    total = 0.0
    numerator = 0.0
    if state is not None:
        numerator, before, total = state
        highest = jnp.maximum(highest, before)
        rescale = jnp.exp(before - highest)
        total = total * rescale
        numerator = numerator * rescale
    for s, kv in zip(scores, pairs):
        powers = jnp.exp(s - highest)
        total = total + jnp.sum(powers, axis=-1, keepdims=True)
        numerator = numerator + jnp.dot(powers.astype(BF16), kv[1], preferred_element_type=F32)
    return numerator, highest, total


def begin_kernel(parts, *refs):
    pairs = refs[PARTS : PARTS + parts]
    outs = refs[PARTS + parts :]
    for part in range(PARTS):
        result = partial_softmax(refs[part][0], pairs, None)
        for out_ref, array in zip(outs[3 * part : 3 * part + 3], result):
            out_ref[...] = jnp.broadcast_to(array, out_ref.shape)


def begin(queries, pairs, head):
    _, rows, width = queries[0].shape
    whole = [pl.BlockSpec((a.shape[0], a.shape[1], head), lambda h: (0, 0, h)) for a in (*queries, *pairs)]
    return pl.pallas_call(
        functools.partial(begin_kernel, len(pairs)),
        grid=(width // head,),
        in_specs=whole,
        out_specs=[pl.BlockSpec((rows, head), lambda h: (0, h))] * (3 * PARTS),
        out_shape=[jax.ShapeDtypeStruct((rows, width), F32)] * (3 * PARTS),
        name="attend_begin",
    )(*queries, *pairs)


def finish_kernel(parts, *refs):
    pairs = refs[4 * PARTS : 4 * PARTS + parts]
    outs = refs[4 * PARTS + parts :]
    for part in range(PARTS):
        numerator_ref, highest_ref, total_ref = refs[PARTS + 3 * part : PARTS + 3 * part + 3]
        state = (numerator_ref[...], highest_ref[:, :1], total_ref[:, :1])
        numerator, _, total = partial_softmax(refs[part][0], pairs, state)
        outs[part][...] = (numerator / total).astype(BF16)


def finish(queries, states, pairs, head):
    _, rows, width = queries[0].shape
    spec = pl.BlockSpec((rows, head), lambda h: (0, h))
    whole = [pl.BlockSpec((a.shape[0], a.shape[1], head), lambda h: (0, 0, h)) for a in (*queries, *pairs)]
    return pl.pallas_call(
        functools.partial(finish_kernel, len(pairs)),
        grid=(width // head,),
        in_specs=whole[:PARTS] + [spec] * (3 * PARTS) + whole[PARTS:],
        out_specs=[spec] * PARTS,
        out_shape=[jax.ShapeDtypeStruct((rows, width), BF16)] * PARTS,
        name="attend_finish",
    )(*queries, *states, *pairs)


def mix_kernel(count, place_ref, *refs):
    each = 2 * count - 1
    blocks = refs[: PARTS * each]
    weight_ref = refs[PARTS * each]
    outs = refs[PARTS * each + 1 : PARTS * each + 1 + count]
    block_ref, sums_ref = refs[PARTS * each + 1 + count :]
    step = pl.program_id(0)
    place = place_ref[0]
    rows = blocks[0].shape[0]
    for d in range(1 - count, count):

        @pl.when(place - step == d)
        def _(d=d):
            for part in range(PARTS):
                block_ref[part * rows : (part + 1) * rows] = blocks[part * each + d + count - 1][...]

    sums = jnp.dot(block_ref[...], weight_ref[...], preferred_element_type=F32)

    @pl.when(step == 0)
    def _():
        sums_ref[...] = sums

    @pl.when(step != 0)
    def _():
        sums_ref[...] += sums

    @pl.when(step == count - 1)
    def _():
        own = rows // count
        for d in range(count):
            owner = lax.rem(place + d, count)
            for part in range(PARTS):
                start = pl.multiple_of(part * rows + owner * own, own)
                outs[d][part * own : (part + 1) * own] = sums_ref[pl.ds(start, own)].astype(BF16)


def mix(place, parts, weight, count):
    rows, width = parts[0][0].shape
    columns = weight.shape[1]
    blocks = [found[d] for found in parts for d in range(1 - count, count)]
    total = PARTS * rows
    return pl.pallas_call(
        functools.partial(mix_kernel, count),
        grid_spec=pltpu.PrefetchScalarGridSpec(
            num_scalar_prefetch=1,
            grid=(count,),
            in_specs=[pl.BlockSpec((rows, width), lambda s, p: (0, 0))] * len(blocks)
            + [pl.BlockSpec((width, columns), lambda s, p: (s, 0))],
            out_specs=[pl.BlockSpec((total // count, columns), lambda s, p: (0, 0))] * count,
            scratch_shapes=[pltpu.VMEM((total, width), BF16), pltpu.VMEM((total, columns), F32)],
        ),
        out_shape=[jax.ShapeDtypeStruct((total // count, columns), BF16)] * count,
        name="mix",
    )(place, *blocks, weight)


def gate_kernel(count, place_ref, tokens_ref, gate_ref, *refs):
    out_ref = refs[-1]
    columns = refs[0].shape[1]
    for d in range(count):
        source = lax.rem(place_ref[0] - d + count, count)
        here = pl.ds(pl.multiple_of(source * columns, columns), columns)
        branch = refs[d][...].astype(F32)
        out_ref[:, here] = (
            tokens_ref[:, here].astype(F32) + gate_ref[:, here] * branch
        ).astype(BF16)


def gated(place, tokens, gate, branches, count):
    whole = pl.BlockSpec(memory_space=pltpu.VMEM)
    return pl.pallas_call(
        functools.partial(gate_kernel, count),
        in_specs=[pl.BlockSpec(memory_space=pltpu.SMEM)] + [whole] * (2 + len(branches)),
        out_specs=whole,
        out_shape=jax.ShapeDtypeStruct(tokens.shape, BF16),
        name="gated",
    )(place, tokens, gate[None], *branches)


def paired(blocks, group, tokens, mod_shift, mod_scale, mod_gate, qkv_weight, query_gain, key_gain, out_weight):
    head = query_gain.shape[0]
    core = lax.axis_index("blk") % 2
    core_list = core.astype(jnp.int32)[None]
    place = lax.axis_index("ulysses").astype(jnp.int32)[None]

    def across(array, mask):
        return lax.ppermute(array, "blk", [(i, i ^ mask) for i in range(blocks)])

    parts = [chains(block, "ulysses", group) for block in modulate(tokens, mod_shift, mod_scale)]
    keep, send, rows = project(core_list, place, parts, qkv_weight, key_gain, group)
    other = across(send, 1)
    keep_x, keep_y = across(keep, 2), across(keep, 4)
    other_x, other_y = across(other, 2), across(other, 4)
    q_keep, q_send = project_query(core_list, rows, qkv_weight, query_gain)
    queries = [q_keep, across(q_send, 1)]
    far = [across(keep_x, 4), across(other_y, 2)]
    states = begin(queries, [keep, other, keep_x, keep_y, other_x, other_y], head)
    mine, returned = finish(queries, states, far, head)
    theirs = across(returned, 1)
    parts = []
    half = mine.shape[0] // PARTS
    for part in range(PARTS):
        a, b = (t[part * half : (part + 1) * half] for t in (mine, theirs))
        attended = jnp.where(
            core == 0, jnp.concatenate([a, b], axis=1), jnp.concatenate([b, a], axis=1)
        )
        parts.append(chains(attended, "ulysses", group))
    columns = mix(place, parts, out_weight, group)
    branches = [columns[0]]
    for d in range(1, group):
        shift = [(i, (i + d) % group) for i in range(group)]
        branches.append(lax.ppermute(columns[d], "ulysses", shift))
    return gated(place, tokens, mod_gate, branches, group)


def head_norm(projected, gain, factor):
    split = projected.reshape(projected.shape[0], -1, gain.shape[0])
    meansq = jnp.mean(split * split, axis=-1, keepdims=True)
    return (split * lax.rsqrt(meansq + 1e-06) * gain * factor).reshape(projected.shape)


def local(tokens, mod_shift, mod_scale, mod_gate, qkv_weight, query_gain, key_gain, out_weight):
    wide = tokens.astype(jnp.float32)
    center = jnp.mean(wide, axis=-1, keepdims=True)
    spread = jnp.mean((wide - center) ** 2, axis=-1, keepdims=True)
    normed = (wide - center) / jnp.sqrt(spread + 1e-06)
    modulated = (normed * (1.0 + mod_scale) + mod_shift).astype(jnp.bfloat16)
    head_size = query_gain.shape[0]
    local_width = qkv_weight.shape[2]
    heads_here = local_width // head_size
    factor = 1.0 / math.sqrt(head_size)
    sums = jnp.einsum(
        "rd,jde->jre",
        lax.all_gather(modulated, "ulysses", axis=0, tiled=True),
        qkv_weight,
        preferred_element_type=jnp.float32,
    )
    queries = head_norm(sums[0], query_gain, factor)
    keys = head_norm(sums[1], key_gain, 1.0)
    stacked = jnp.stack([queries, keys, sums[2]]).astype(jnp.bfloat16)
    queries, keys, values = (stacked[0], stacked[1], stacked[2])
    query_rows = queries.shape[0]
    query_heads = queries.reshape(query_rows, heads_here, head_size)
    start_state = (
        jnp.full((heads_here, query_rows), -1e30, jnp.float32),
        jnp.zeros((heads_here, query_rows), jnp.float32),
        jnp.zeros((heads_here, query_rows, head_size), jnp.float32),
    )
    key_part = lax.all_gather(keys, "blk", axis=0, tiled=True)
    value_part = lax.all_gather(values, "blk", axis=0, tiled=True)
    count = key_part.shape[0] // query_rows

    def step(position, state):
        highest, total, numerator = state
        key_block = lax.dynamic_slice_in_dim(key_part, position * query_rows, query_rows, 0)
        value_block = lax.dynamic_slice_in_dim(value_part, position * query_rows, query_rows, 0)
        key_block = key_block.reshape(query_rows, heads_here, head_size)
        value_block = value_block.reshape(query_rows, heads_here, head_size)
        scores = jnp.einsum(
            "qhd,khd->hqk", query_heads, key_block, preferred_element_type=jnp.float32
        )
        new_high = jnp.maximum(highest, jnp.max(scores, axis=-1))
        rescale = jnp.exp(highest - new_high)
        powers = jnp.exp(scores - new_high[..., None])
        total = total * rescale + jnp.sum(powers, axis=-1)
        numerator = numerator * rescale[..., None] + jnp.einsum(
            "hqk,khd->hqd",
            powers.astype(jnp.bfloat16),
            value_block,
            preferred_element_type=jnp.float32,
        )
        return (new_high, total, numerator)

    highest, total, numerator = lax.fori_loop(0, count, step, start_state)
    attended = (numerator / total[..., None]).transpose(1, 0, 2).reshape(query_rows, local_width)
    attended = attended.astype(jnp.bfloat16)
    columns = jnp.dot(
        lax.all_gather(attended, "ulysses", axis=1, tiled=True),
        out_weight,
        preferred_element_type=jnp.float32,
    )
    branch = lax.all_to_all(
        columns.astype(jnp.bfloat16), "ulysses", split_axis=0, concat_axis=1, tiled=True
    ).astype(columns.dtype)
    return (wide + mod_gate * branch).astype(jnp.bfloat16)


def solution(mesh):
    in_specs = (
        P(("blk", "ulysses"), None),
        P(),
        P(),
        P(),
        P(None, None, "ulysses"),
        P(),
        P(),
        P(None, "ulysses"),
    )
    out_specs = P(("blk", "ulysses"), None)
    blocks, group = mesh.shape["blk"], mesh.shape["ulysses"]

    def body(*args):
        tokens, head, width = args[0], args[5].shape[0], args[4].shape[2]
        pairs_split = width % (2 * head) == 0 and tokens.shape[0] % (16 * PARTS) == 0
        if blocks == 8 and pairs_split:
            return paired(blocks, group, *args)
        return local(*args)

    return jax.shard_map(body, mesh=mesh, in_specs=in_specs, out_specs=out_specs, check_vma=False)
```

```python
import functools
import math

import jax
import jax.numpy as jnp
from jax import lax
from jax.experimental import pallas as pl
from jax.experimental.pallas import tpu as pltpu
from jax.sharding import PartitionSpec as P


F32 = jnp.float32
BF16 = jnp.bfloat16
PARTS = 2


def norm_kernel(tokens_ref, shift_ref, scale_ref, *out_refs):
    rows = out_refs[0].shape[0]
    for part, out_ref in enumerate(out_refs):
        wide = tokens_ref[part * rows : (part + 1) * rows].astype(F32)
        center = jnp.mean(wide, axis=-1, keepdims=True)
        spread = jnp.mean((wide - center) ** 2, axis=-1, keepdims=True)
        normed = (wide - center) / jnp.sqrt(spread + 1e-06)
        out_ref[...] = (normed * (1.0 + scale_ref[...]) + shift_ref[...]).astype(BF16)


def modulate(tokens, shift, scale):
    shape = (tokens.shape[0] // PARTS, tokens.shape[1])
    return pl.pallas_call(
        norm_kernel,
        out_shape=[jax.ShapeDtypeStruct(shape, BF16)] * PARTS,
        name="modulate",
    )(tokens, shift[None], scale[None])


def chains(block, axis, count):
    found = {0: block}
    for hop in range(1, count):
        up = [(i, i + 1) for i in range(hop - 1, count - 1)]
        down = [(count - 1 - a, count - 1 - b) for a, b in up]
        found[hop] = lax.ppermute(found[hop - 1], axis, up)
        found[-hop] = lax.ppermute(found[1 - hop], axis, down)
    return found


def project_kernel(count, head, factor, core_ref, place_ref, *refs):
    blocks = refs[: PARTS * (2 * count - 1)]
    weight_ref, gains_ref, keep_ref, send_ref, rows_ref = refs[len(blocks) :]
    job = pl.program_id(0)
    each = blocks[0].shape[0]

    @pl.when(job == 0)
    def _():
        for part in range(PARTS):
            for place in range(count):

                @pl.when(place_ref[0] == place)
                def _(part=part, place=place):
                    for s in range(count):
                        start = (part * count + s) * each
                        block = blocks[part * (2 * count - 1) + place - s + count - 1]
                        rows_ref[start : start + each] = block[...]

    sums = jnp.dot(rows_ref[...], weight_ref[0], preferred_element_type=F32)
    finish_projection(job, sums, head, factor, core_ref, gains_ref, keep_ref, send_ref)


def again_kernel(head, factor, core_ref, rows_ref, weight_ref, gains_ref, keep_ref, send_ref):
    sums = jnp.dot(rows_ref[...], weight_ref[0], preferred_element_type=F32)
    finish_projection(0, sums, head, factor, core_ref, gains_ref, keep_ref, send_ref)


def finish_projection(job, sums, head, factor, core_ref, gains_ref, keep_ref, send_ref):
    half = sums.shape[1] // 2
    heads = half // head

    def store(pieces):
        for core in range(2):

            @pl.when(core_ref[0] == core)
            def _(core=core):
                for out_ref, side in ((keep_ref, core), (send_ref, 1 - core)):
                    for h in range(heads):
                        out_ref[0, :, h * head : (h + 1) * head] = pieces[side * heads + h]

    pieces = [sums[:, h * head : (h + 1) * head] for h in range(2 * heads)]

    def normed():
        out = []
        for piece in pieces:
            meansq = jnp.mean(piece * piece, axis=-1, keepdims=True)
            out.append((piece * lax.rsqrt(meansq + 1e-06) * gains_ref[...] * factor).astype(BF16))
        return out

    if isinstance(job, int):
        store(normed())
    else:

        @pl.when(job == 0)
        def _():
            store(normed())

        @pl.when(job != 0)
        def _():
            store([piece.astype(BF16) for piece in pieces])


def project(core, place, parts, weight, gain, count):
    each, depth = parts[0][0].shape
    width = weight.shape[2]
    rows = PARTS * count * each
    blocks = [found[d] for found in parts for d in range(1 - count, count)]
    kept = pl.BlockSpec((1, rows, width // 2), lambda j, c, p: (j, 0, 0))
    return pl.pallas_call(
        functools.partial(project_kernel, count, gain.shape[0], 1.0),
        grid_spec=pltpu.PrefetchScalarGridSpec(
            num_scalar_prefetch=2,
            grid=(2,),
            in_specs=[pl.BlockSpec((each, depth), lambda j, c, p: (0, 0))] * len(blocks)
            + [
                pl.BlockSpec((1, depth, width), lambda j, c, p: (j + 1, 0, 0)),
                pl.BlockSpec((1, gain.shape[0]), lambda j, c, p: (0, 0)),
            ],
            out_specs=[kept, kept, pl.BlockSpec((rows, depth), lambda j, c, p: (0, 0))],
        ),
        out_shape=[jax.ShapeDtypeStruct((2, rows, width // 2), BF16)] * 2
        + [jax.ShapeDtypeStruct((rows, depth), BF16)],
        name="project_kv",
    )(core, place, *blocks, weight, gain[None])


def project_query(core, rows, weight, gain):
    count, depth = rows.shape
    width = weight.shape[2]
    kept = pl.BlockSpec((1, count, width // 2), lambda j, c: (0, 0, 0))
    return pl.pallas_call(
        functools.partial(again_kernel, gain.shape[0], 1.0 / math.sqrt(gain.shape[0])),
        grid_spec=pltpu.PrefetchScalarGridSpec(
            num_scalar_prefetch=1,
            grid=(1,),
            in_specs=[
                pl.BlockSpec((count, depth), lambda j, c: (0, 0)),
                pl.BlockSpec((1, depth, width), lambda j, c: (0, 0, 0)),
                pl.BlockSpec((1, gain.shape[0]), lambda j, c: (0, 0)),
            ],
            out_specs=[kept, kept],
        ),
        out_shape=[jax.ShapeDtypeStruct((1, count, width // 2), BF16)] * 2,
        name="project_q",
    )(core, rows, weight, gain[None])


def partial_softmax(query, pairs, state):
    scores = [
        lax.dot_general(query, kv[0], (((1,), (1,)), ((), ())), preferred_element_type=F32)
        for kv in pairs
    ]
    highest = functools.reduce(jnp.maximum, [jnp.max(s, axis=-1, keepdims=True) for s in scores])
    total = 0.0
    numerator = 0.0
    if state is not None:
        numerator, before, total = state
        highest = jnp.maximum(highest, before)
        rescale = jnp.exp(before - highest)
        total = total * rescale
        numerator = numerator * rescale
    for s, kv in zip(scores, pairs):
        powers = jnp.exp(s - highest)
        total = total + jnp.sum(powers, axis=-1, keepdims=True)
        numerator = numerator + jnp.dot(powers.astype(BF16), kv[1], preferred_element_type=F32)
    return numerator, highest, total


def begin_kernel(parts, *refs):
    pairs = refs[PARTS : PARTS + parts]
    outs = refs[PARTS + parts :]
    for part in range(PARTS):
        result = partial_softmax(refs[part][0], pairs, None)
        for out_ref, array in zip(outs[3 * part : 3 * part + 3], result):
            out_ref[...] = jnp.broadcast_to(array, out_ref.shape)


def begin(queries, pairs, head):
    _, rows, width = queries[0].shape
    whole = [pl.BlockSpec((a.shape[0], a.shape[1], head), lambda h: (0, 0, h)) for a in (*queries, *pairs)]
    return pl.pallas_call(
        functools.partial(begin_kernel, len(pairs)),
        grid=(width // head,),
        in_specs=whole,
        out_specs=[pl.BlockSpec((rows, head), lambda h: (0, h))] * (3 * PARTS),
        out_shape=[jax.ShapeDtypeStruct((rows, width), F32)] * (3 * PARTS),
        name="attend_begin",
    )(*queries, *pairs)


def finish_kernel(parts, *refs):
    pairs = refs[4 * PARTS : 4 * PARTS + parts]
    outs = refs[4 * PARTS + parts :]
    for part in range(PARTS):
        numerator_ref, highest_ref, total_ref = refs[PARTS + 3 * part : PARTS + 3 * part + 3]
        state = (numerator_ref[...], highest_ref[:, :1], total_ref[:, :1])
        numerator, _, total = partial_softmax(refs[part][0], pairs, state)
        outs[part][...] = (numerator / total).astype(BF16)


def finish(queries, states, pairs, head):
    _, rows, width = queries[0].shape
    spec = pl.BlockSpec((rows, head), lambda h: (0, h))
    whole = [pl.BlockSpec((a.shape[0], a.shape[1], head), lambda h: (0, 0, h)) for a in (*queries, *pairs)]
    return pl.pallas_call(
        functools.partial(finish_kernel, len(pairs)),
        grid=(width // head,),
        in_specs=whole[:PARTS] + [spec] * (3 * PARTS) + whole[PARTS:],
        out_specs=[spec] * PARTS,
        out_shape=[jax.ShapeDtypeStruct((rows, width), BF16)] * PARTS,
        name="attend_finish",
    )(*queries, *states, *pairs)


def mix_kernel(count, place_ref, *refs):
    each = 2 * count - 1
    blocks = refs[: PARTS * each]
    weight_ref = refs[PARTS * each]
    outs = refs[PARTS * each + 1 : PARTS * each + 1 + count]
    block_ref, sums_ref = refs[PARTS * each + 1 + count :]
    step = pl.program_id(0)
    place = place_ref[0]
    rows = blocks[0].shape[0]
    for d in range(1 - count, count):

        @pl.when(place - step == d)
        def _(d=d):
            for part in range(PARTS):
                block_ref[part * rows : (part + 1) * rows] = blocks[part * each + d + count - 1][...]

    sums = jnp.dot(block_ref[...], weight_ref[...], preferred_element_type=F32)

    @pl.when(step == 0)
    def _():
        sums_ref[...] = sums

    @pl.when(step != 0)
    def _():
        sums_ref[...] += sums

    @pl.when(step == count - 1)
    def _():
        own = rows // count
        for d in range(count):
            owner = lax.rem(place + d, count)
            for part in range(PARTS):
                start = pl.multiple_of(part * rows + owner * own, own)
                outs[d][part * own : (part + 1) * own] = sums_ref[pl.ds(start, own)].astype(BF16)


def mix(place, parts, weight, count):
    rows, width = parts[0][0].shape
    columns = weight.shape[1]
    blocks = [found[d] for found in parts for d in range(1 - count, count)]
    total = PARTS * rows
    return pl.pallas_call(
        functools.partial(mix_kernel, count),
        grid_spec=pltpu.PrefetchScalarGridSpec(
            num_scalar_prefetch=1,
            grid=(count,),
            in_specs=[pl.BlockSpec((rows, width), lambda s, p: (0, 0))] * len(blocks)
            + [pl.BlockSpec((width, columns), lambda s, p: (s, 0))],
            out_specs=[pl.BlockSpec((total // count, columns), lambda s, p: (0, 0))] * count,
            scratch_shapes=[pltpu.VMEM((total, width), BF16), pltpu.VMEM((total, columns), F32)],
        ),
        out_shape=[jax.ShapeDtypeStruct((total // count, columns), BF16)] * count,
        name="mix",
    )(place, *blocks, weight)


def gate_kernel(count, place_ref, tokens_ref, gate_ref, *refs):
    out_ref = refs[-1]
    columns = refs[0].shape[1]
    for d in range(count):
        source = lax.rem(place_ref[0] - d + count, count)
        here = pl.ds(pl.multiple_of(source * columns, columns), columns)
        branch = refs[d][...].astype(F32)
        out_ref[:, here] = (
            tokens_ref[:, here].astype(F32) + gate_ref[:, here] * branch
        ).astype(BF16)


def gated(place, tokens, gate, branches, count):
    whole = pl.BlockSpec(memory_space=pltpu.VMEM)
    return pl.pallas_call(
        functools.partial(gate_kernel, count),
        in_specs=[pl.BlockSpec(memory_space=pltpu.SMEM)] + [whole] * (2 + len(branches)),
        out_specs=whole,
        out_shape=jax.ShapeDtypeStruct(tokens.shape, BF16),
        name="gated",
    )(place, tokens, gate[None], *branches)


def paired(blocks, group, tokens, mod_shift, mod_scale, mod_gate, qkv_weight, query_gain, key_gain, out_weight):
    head = query_gain.shape[0]
    core = lax.axis_index("blk") % 2
    core_list = core.astype(jnp.int32)[None]
    place = lax.axis_index("ulysses").astype(jnp.int32)[None]

    def across(array, mask):
        return lax.ppermute(array, "blk", [(i, i ^ mask) for i in range(blocks)])

    parts = [chains(block, "ulysses", group) for block in modulate(tokens, mod_shift, mod_scale)]
    keep, send, rows = project(core_list, place, parts, qkv_weight, key_gain, group)
    other = across(send, 1)
    keep_x, keep_y = across(keep, 2), across(keep, 4)
    other_x, other_y = across(other, 2), across(other, 4)
    q_keep, q_send = project_query(core_list, rows, qkv_weight, query_gain)
    queries = [q_keep, across(q_send, 1)]
    onward, _ = lax.optimization_barrier((keep_x, q_send))
    far = [across(onward, 4), across(other_y, 2)]
    states = begin(queries, [keep, other, keep_x, keep_y, other_x, other_y], head)
    mine, returned = finish(queries, states, far, head)
    theirs = across(returned, 1)
    parts = []
    half = mine.shape[0] // PARTS
    for part in range(PARTS):
        a, b = (t[part * half : (part + 1) * half] for t in (mine, theirs))
        attended = jnp.where(
            core == 0, jnp.concatenate([a, b], axis=1), jnp.concatenate([b, a], axis=1)
        )
        parts.append(chains(attended, "ulysses", group))
    columns = mix(place, parts, out_weight, group)
    branches = [columns[0]]
    for d in range(1, group):
        shift = [(i, (i + d) % group) for i in range(group)]
        branches.append(lax.ppermute(columns[d], "ulysses", shift))
    return gated(place, tokens, mod_gate, branches, group)


def head_norm(projected, gain, factor):
    split = projected.reshape(projected.shape[0], -1, gain.shape[0])
    meansq = jnp.mean(split * split, axis=-1, keepdims=True)
    return (split * lax.rsqrt(meansq + 1e-06) * gain * factor).reshape(projected.shape)


def local(tokens, mod_shift, mod_scale, mod_gate, qkv_weight, query_gain, key_gain, out_weight):
    wide = tokens.astype(jnp.float32)
    center = jnp.mean(wide, axis=-1, keepdims=True)
    spread = jnp.mean((wide - center) ** 2, axis=-1, keepdims=True)
    normed = (wide - center) / jnp.sqrt(spread + 1e-06)
    modulated = (normed * (1.0 + mod_scale) + mod_shift).astype(jnp.bfloat16)
    head_size = query_gain.shape[0]
    local_width = qkv_weight.shape[2]
    heads_here = local_width // head_size
    factor = 1.0 / math.sqrt(head_size)
    sums = jnp.einsum(
        "rd,jde->jre",
        lax.all_gather(modulated, "ulysses", axis=0, tiled=True),
        qkv_weight,
        preferred_element_type=jnp.float32,
    )
    queries = head_norm(sums[0], query_gain, factor)
    keys = head_norm(sums[1], key_gain, 1.0)
    stacked = jnp.stack([queries, keys, sums[2]]).astype(jnp.bfloat16)
    queries, keys, values = (stacked[0], stacked[1], stacked[2])
    query_rows = queries.shape[0]
    query_heads = queries.reshape(query_rows, heads_here, head_size)
    start_state = (
        jnp.full((heads_here, query_rows), -1e30, jnp.float32),
        jnp.zeros((heads_here, query_rows), jnp.float32),
        jnp.zeros((heads_here, query_rows, head_size), jnp.float32),
    )
    key_part = lax.all_gather(keys, "blk", axis=0, tiled=True)
    value_part = lax.all_gather(values, "blk", axis=0, tiled=True)
    count = key_part.shape[0] // query_rows

    def step(position, state):
        highest, total, numerator = state
        key_block = lax.dynamic_slice_in_dim(key_part, position * query_rows, query_rows, 0)
        value_block = lax.dynamic_slice_in_dim(value_part, position * query_rows, query_rows, 0)
        key_block = key_block.reshape(query_rows, heads_here, head_size)
        value_block = value_block.reshape(query_rows, heads_here, head_size)
        scores = jnp.einsum(
            "qhd,khd->hqk", query_heads, key_block, preferred_element_type=jnp.float32
        )
        new_high = jnp.maximum(highest, jnp.max(scores, axis=-1))
        rescale = jnp.exp(highest - new_high)
        powers = jnp.exp(scores - new_high[..., None])
        total = total * rescale + jnp.sum(powers, axis=-1)
        numerator = numerator * rescale[..., None] + jnp.einsum(
            "hqk,khd->hqd",
            powers.astype(jnp.bfloat16),
            value_block,
            preferred_element_type=jnp.float32,
        )
        return (new_high, total, numerator)

    highest, total, numerator = lax.fori_loop(0, count, step, start_state)
    attended = (numerator / total[..., None]).transpose(1, 0, 2).reshape(query_rows, local_width)
    attended = attended.astype(jnp.bfloat16)
    columns = jnp.dot(
        lax.all_gather(attended, "ulysses", axis=1, tiled=True),
        out_weight,
        preferred_element_type=jnp.float32,
    )
    branch = lax.all_to_all(
        columns.astype(jnp.bfloat16), "ulysses", split_axis=0, concat_axis=1, tiled=True
    ).astype(columns.dtype)
    return (wide + mod_gate * branch).astype(jnp.bfloat16)


def solution(mesh):
    in_specs = (
        P(("blk", "ulysses"), None),
        P(),
        P(),
        P(),
        P(None, None, "ulysses"),
        P(),
        P(),
        P(None, "ulysses"),
    )
    out_specs = P(("blk", "ulysses"), None)
    blocks, group = mesh.shape["blk"], mesh.shape["ulysses"]

    def body(*args):
        tokens, head, width = args[0], args[5].shape[0], args[4].shape[2]
        pairs_split = width % (2 * head) == 0 and tokens.shape[0] % (16 * PARTS) == 0
        if blocks == 8 and pairs_split:
            return paired(blocks, group, *args)
        return local(*args)

    return jax.shard_map(body, mesh=mesh, in_specs=in_specs, out_specs=out_specs, check_vma=False)
```

```python
import functools
import math

import jax
import jax.numpy as jnp
from jax import lax
from jax.experimental import pallas as pl
from jax.experimental.pallas import tpu as pltpu
from jax.sharding import PartitionSpec as P


F32 = jnp.float32
BF16 = jnp.bfloat16
PARTS = 2


def norm_kernel(tokens_ref, shift_ref, scale_ref, *out_refs):
    rows = out_refs[0].shape[0]
    for part, out_ref in enumerate(out_refs):
        wide = tokens_ref[part * rows : (part + 1) * rows].astype(F32)
        center = jnp.mean(wide, axis=-1, keepdims=True)
        spread = jnp.mean((wide - center) ** 2, axis=-1, keepdims=True)
        normed = (wide - center) / jnp.sqrt(spread + 1e-06)
        out_ref[...] = (normed * (1.0 + scale_ref[...]) + shift_ref[...]).astype(BF16)


def modulate(tokens, shift, scale):
    shape = (tokens.shape[0] // PARTS, tokens.shape[1])
    return pl.pallas_call(
        norm_kernel,
        out_shape=[jax.ShapeDtypeStruct(shape, BF16)] * PARTS,
        name="modulate",
    )(tokens, shift[None], scale[None])


def chains(block, axis, count):
    found = {0: block}
    for hop in range(1, count):
        up = [(i, i + 1) for i in range(hop - 1, count - 1)]
        down = [(count - 1 - a, count - 1 - b) for a, b in up]
        found[hop] = lax.ppermute(found[hop - 1], axis, up)
        found[-hop] = lax.ppermute(found[1 - hop], axis, down)
    return found


def project_kernel(count, head, factor, core_ref, place_ref, *refs):
    blocks = refs[: PARTS * (2 * count - 1)]
    weight_ref, gains_ref, keep_ref, send_ref, rows_ref = refs[len(blocks) :]
    job = pl.program_id(0)
    each = blocks[0].shape[0]

    @pl.when(job == 0)
    def _():
        for part in range(PARTS):
            for place in range(count):

                @pl.when(place_ref[0] == place)
                def _(part=part, place=place):
                    for s in range(count):
                        start = (part * count + s) * each
                        block = blocks[part * (2 * count - 1) + place - s + count - 1]
                        rows_ref[start : start + each] = block[...]

    sums = jnp.dot(rows_ref[...], weight_ref[0], preferred_element_type=F32)
    finish_projection(job, sums, head, factor, core_ref, gains_ref, keep_ref, send_ref)


def again_kernel(head, factor, core_ref, rows_ref, weight_ref, gains_ref, keep_ref, send_ref):
    sums = jnp.dot(rows_ref[...], weight_ref[0], preferred_element_type=F32)
    finish_projection(0, sums, head, factor, core_ref, gains_ref, keep_ref, send_ref)


def finish_projection(job, sums, head, factor, core_ref, gains_ref, keep_ref, send_ref):
    half = sums.shape[1] // 2
    heads = half // head

    def store(pieces):
        for core in range(2):

            @pl.when(core_ref[0] == core)
            def _(core=core):
                for out_ref, side in ((keep_ref, core), (send_ref, 1 - core)):
                    for h in range(heads):
                        out_ref[0, :, h * head : (h + 1) * head] = pieces[side * heads + h]

    pieces = [sums[:, h * head : (h + 1) * head] for h in range(2 * heads)]

    def normed():
        out = []
        for piece in pieces:
            meansq = jnp.mean(piece * piece, axis=-1, keepdims=True)
            out.append((piece * lax.rsqrt(meansq + 1e-06) * gains_ref[...] * factor).astype(BF16))
        return out

    if isinstance(job, int):
        store(normed())
    else:

        @pl.when(job == 0)
        def _():
            store(normed())

        @pl.when(job != 0)
        def _():
            store([piece.astype(BF16) for piece in pieces])


def project(core, place, parts, weight, gain, count):
    each, depth = parts[0][0].shape
    width = weight.shape[2]
    rows = PARTS * count * each
    blocks = [found[d] for found in parts for d in range(1 - count, count)]
    kept = pl.BlockSpec((1, rows, width // 2), lambda j, c, p: (j, 0, 0))
    return pl.pallas_call(
        functools.partial(project_kernel, count, gain.shape[0], 1.0),
        grid_spec=pltpu.PrefetchScalarGridSpec(
            num_scalar_prefetch=2,
            grid=(2,),
            in_specs=[pl.BlockSpec((each, depth), lambda j, c, p: (0, 0))] * len(blocks)
            + [
                pl.BlockSpec((1, depth, width), lambda j, c, p: (j + 1, 0, 0)),
                pl.BlockSpec((1, gain.shape[0]), lambda j, c, p: (0, 0)),
            ],
            out_specs=[kept, kept, pl.BlockSpec((rows, depth), lambda j, c, p: (0, 0))],
        ),
        out_shape=[jax.ShapeDtypeStruct((2, rows, width // 2), BF16)] * 2
        + [jax.ShapeDtypeStruct((rows, depth), BF16)],
        name="project_kv",
    )(core, place, *blocks, weight, gain[None])


def project_query(core, rows, weight, gain):
    count, depth = rows.shape
    width = weight.shape[2]
    kept = pl.BlockSpec((1, count, width // 2), lambda j, c: (0, 0, 0))
    return pl.pallas_call(
        functools.partial(again_kernel, gain.shape[0], 1.0 / math.sqrt(gain.shape[0])),
        grid_spec=pltpu.PrefetchScalarGridSpec(
            num_scalar_prefetch=1,
            grid=(1,),
            in_specs=[
                pl.BlockSpec((count, depth), lambda j, c: (0, 0)),
                pl.BlockSpec((1, depth, width), lambda j, c: (0, 0, 0)),
                pl.BlockSpec((1, gain.shape[0]), lambda j, c: (0, 0)),
            ],
            out_specs=[kept, kept],
        ),
        out_shape=[jax.ShapeDtypeStruct((1, count, width // 2), BF16)] * 2,
        name="project_q",
    )(core, rows, weight, gain[None])


def partial_softmax(query, pairs, state):
    scores = [
        lax.dot_general(query, kv[0], (((1,), (1,)), ((), ())), preferred_element_type=F32)
        for kv in pairs
    ]
    highest = functools.reduce(jnp.maximum, [jnp.max(s, axis=-1, keepdims=True) for s in scores])
    total = 0.0
    numerator = 0.0
    if state is not None:
        numerator, before, total = state
        highest = jnp.maximum(highest, before)
        rescale = jnp.exp(before - highest)
        total = total * rescale
        numerator = numerator * rescale
    for s, kv in zip(scores, pairs):
        powers = jnp.exp(s - highest)
        total = total + jnp.sum(powers, axis=-1, keepdims=True)
        numerator = numerator + jnp.dot(powers.astype(BF16), kv[1], preferred_element_type=F32)
    return numerator, highest, total


def begin_kernel(parts, *refs):
    pairs = refs[PARTS : PARTS + parts]
    outs = refs[PARTS + parts :]
    for part in range(PARTS):
        result = partial_softmax(refs[part][0], pairs, None)
        for out_ref, array in zip(outs[3 * part : 3 * part + 3], result):
            out_ref[...] = jnp.broadcast_to(array, out_ref.shape)


def begin(queries, pairs, head):
    _, rows, width = queries[0].shape
    whole = [pl.BlockSpec((a.shape[0], a.shape[1], head), lambda h: (0, 0, h)) for a in (*queries, *pairs)]
    return pl.pallas_call(
        functools.partial(begin_kernel, len(pairs)),
        grid=(width // head,),
        in_specs=whole,
        out_specs=[pl.BlockSpec((rows, head), lambda h: (0, h))] * (3 * PARTS),
        out_shape=[jax.ShapeDtypeStruct((rows, width), F32)] * (3 * PARTS),
        name="attend_begin",
    )(*queries, *pairs)


def finish_kernel(parts, *refs):
    pairs = refs[4 * PARTS : 4 * PARTS + parts]
    outs = refs[4 * PARTS + parts :]
    for part in range(PARTS):
        numerator_ref, highest_ref, total_ref = refs[PARTS + 3 * part : PARTS + 3 * part + 3]
        state = (numerator_ref[...], highest_ref[:, :1], total_ref[:, :1])
        numerator, _, total = partial_softmax(refs[part][0], pairs, state)
        outs[part][...] = (numerator / total).astype(BF16)


def finish(queries, states, pairs, head):
    _, rows, width = queries[0].shape
    spec = pl.BlockSpec((rows, head), lambda h: (0, h))
    whole = [pl.BlockSpec((a.shape[0], a.shape[1], head), lambda h: (0, 0, h)) for a in (*queries, *pairs)]
    return pl.pallas_call(
        functools.partial(finish_kernel, len(pairs)),
        grid=(width // head,),
        in_specs=whole[:PARTS] + [spec] * (3 * PARTS) + whole[PARTS:],
        out_specs=[spec] * PARTS,
        out_shape=[jax.ShapeDtypeStruct((rows, width), BF16)] * PARTS,
        name="attend_finish",
    )(*queries, *states, *pairs)


def mix_kernel(count, place_ref, *refs):
    each = 2 * count - 1
    blocks = refs[: PARTS * each]
    weight_ref = refs[PARTS * each]
    outs = refs[PARTS * each + 1 : PARTS * each + 1 + count]
    block_ref, sums_ref = refs[PARTS * each + 1 + count :]
    step = pl.program_id(0)
    place = place_ref[0]
    rows = blocks[0].shape[0]
    for d in range(1 - count, count):

        @pl.when(place - step == d)
        def _(d=d):
            for part in range(PARTS):
                block_ref[part * rows : (part + 1) * rows] = blocks[part * each + d + count - 1][...]

    sums = jnp.dot(block_ref[...], weight_ref[...], preferred_element_type=F32)

    @pl.when(step == 0)
    def _():
        sums_ref[...] = sums

    @pl.when(step != 0)
    def _():
        sums_ref[...] += sums

    @pl.when(step == count - 1)
    def _():
        own = rows // count
        for d in range(count):
            owner = lax.rem(place + d, count)
            for part in range(PARTS):
                start = pl.multiple_of(part * rows + owner * own, own)
                outs[d][part * own : (part + 1) * own] = sums_ref[pl.ds(start, own)].astype(BF16)


def mix(place, parts, weight, count):
    rows, width = parts[0][0].shape
    columns = weight.shape[1]
    blocks = [found[d] for found in parts for d in range(1 - count, count)]
    total = PARTS * rows
    return pl.pallas_call(
        functools.partial(mix_kernel, count),
        grid_spec=pltpu.PrefetchScalarGridSpec(
            num_scalar_prefetch=1,
            grid=(count,),
            in_specs=[pl.BlockSpec((rows, width), lambda s, p: (0, 0))] * len(blocks)
            + [pl.BlockSpec((width, columns), lambda s, p: (s, 0))],
            out_specs=[pl.BlockSpec((total // count, columns), lambda s, p: (0, 0))] * count,
            scratch_shapes=[pltpu.VMEM((total, width), BF16), pltpu.VMEM((total, columns), F32)],
        ),
        out_shape=[jax.ShapeDtypeStruct((total // count, columns), BF16)] * count,
        name="mix",
    )(place, *blocks, weight)


def gate_kernel(count, place_ref, tokens_ref, gate_ref, *refs):
    out_ref = refs[-1]
    columns = refs[0].shape[1]
    for d in range(count):
        source = lax.rem(place_ref[0] - d + count, count)
        here = pl.ds(pl.multiple_of(source * columns, columns), columns)
        branch = refs[d][...].astype(F32)
        out_ref[:, here] = (
            tokens_ref[:, here].astype(F32) + gate_ref[:, here] * branch
        ).astype(BF16)


def gated(place, tokens, gate, branches, count):
    whole = pl.BlockSpec(memory_space=pltpu.VMEM)
    return pl.pallas_call(
        functools.partial(gate_kernel, count),
        in_specs=[pl.BlockSpec(memory_space=pltpu.SMEM)] + [whole] * (2 + len(branches)),
        out_specs=whole,
        out_shape=jax.ShapeDtypeStruct(tokens.shape, BF16),
        name="gated",
    )(place, tokens, gate[None], *branches)


def paired(blocks, group, tokens, mod_shift, mod_scale, mod_gate, qkv_weight, query_gain, key_gain, out_weight):
    head = query_gain.shape[0]
    core = lax.axis_index("blk") % 2
    core_list = core.astype(jnp.int32)[None]
    place = lax.axis_index("ulysses").astype(jnp.int32)[None]

    def across(array, mask):
        return lax.ppermute(array, "blk", [(i, i ^ mask) for i in range(blocks)])

    parts = [chains(block, "ulysses", group) for block in modulate(tokens, mod_shift, mod_scale)]
    keep, send, rows = project(core_list, place, parts, qkv_weight, key_gain, group)
    other = across(send, 1)
    keep_x, keep_y = across(keep, 2), across(keep, 4)
    other_x, other_y = across(other, 2), across(other, 4)
    q_keep, q_send = project_query(core_list, rows, qkv_weight, query_gain)
    queries = [q_keep, across(q_send, 1)]
    onward, _ = lax.optimization_barrier((keep_x, q_send))
    far = [across(onward, 4), across(other_y, 2)]
    states = begin(queries, [keep, other, keep_x, other_y], head)
    mine, returned = finish(queries, states, [keep_y, other_x, *far], head)
    theirs = across(returned, 1)
    parts = []
    half = mine.shape[0] // PARTS
    for part in range(PARTS):
        a, b = (t[part * half : (part + 1) * half] for t in (mine, theirs))
        attended = jnp.where(
            core == 0, jnp.concatenate([a, b], axis=1), jnp.concatenate([b, a], axis=1)
        )
        parts.append(chains(attended, "ulysses", group))
    columns = mix(place, parts, out_weight, group)
    branches = [columns[0]]
    for d in range(1, group):
        shift = [(i, (i + d) % group) for i in range(group)]
        branches.append(lax.ppermute(columns[d], "ulysses", shift))
    return gated(place, tokens, mod_gate, branches, group)


def head_norm(projected, gain, factor):
    split = projected.reshape(projected.shape[0], -1, gain.shape[0])
    meansq = jnp.mean(split * split, axis=-1, keepdims=True)
    return (split * lax.rsqrt(meansq + 1e-06) * gain * factor).reshape(projected.shape)


def local(tokens, mod_shift, mod_scale, mod_gate, qkv_weight, query_gain, key_gain, out_weight):
    wide = tokens.astype(jnp.float32)
    center = jnp.mean(wide, axis=-1, keepdims=True)
    spread = jnp.mean((wide - center) ** 2, axis=-1, keepdims=True)
    normed = (wide - center) / jnp.sqrt(spread + 1e-06)
    modulated = (normed * (1.0 + mod_scale) + mod_shift).astype(jnp.bfloat16)
    head_size = query_gain.shape[0]
    local_width = qkv_weight.shape[2]
    heads_here = local_width // head_size
    factor = 1.0 / math.sqrt(head_size)
    sums = jnp.einsum(
        "rd,jde->jre",
        lax.all_gather(modulated, "ulysses", axis=0, tiled=True),
        qkv_weight,
        preferred_element_type=jnp.float32,
    )
    queries = head_norm(sums[0], query_gain, factor)
    keys = head_norm(sums[1], key_gain, 1.0)
    stacked = jnp.stack([queries, keys, sums[2]]).astype(jnp.bfloat16)
    queries, keys, values = (stacked[0], stacked[1], stacked[2])
    query_rows = queries.shape[0]
    query_heads = queries.reshape(query_rows, heads_here, head_size)
    start_state = (
        jnp.full((heads_here, query_rows), -1e30, jnp.float32),
        jnp.zeros((heads_here, query_rows), jnp.float32),
        jnp.zeros((heads_here, query_rows, head_size), jnp.float32),
    )
    key_part = lax.all_gather(keys, "blk", axis=0, tiled=True)
    value_part = lax.all_gather(values, "blk", axis=0, tiled=True)
    count = key_part.shape[0] // query_rows

    def step(position, state):
        highest, total, numerator = state
        key_block = lax.dynamic_slice_in_dim(key_part, position * query_rows, query_rows, 0)
        value_block = lax.dynamic_slice_in_dim(value_part, position * query_rows, query_rows, 0)
        key_block = key_block.reshape(query_rows, heads_here, head_size)
        value_block = value_block.reshape(query_rows, heads_here, head_size)
        scores = jnp.einsum(
            "qhd,khd->hqk", query_heads, key_block, preferred_element_type=jnp.float32
        )
        new_high = jnp.maximum(highest, jnp.max(scores, axis=-1))
        rescale = jnp.exp(highest - new_high)
        powers = jnp.exp(scores - new_high[..., None])
        total = total * rescale + jnp.sum(powers, axis=-1)
        numerator = numerator * rescale[..., None] + jnp.einsum(
            "hqk,khd->hqd",
            powers.astype(jnp.bfloat16),
            value_block,
            preferred_element_type=jnp.float32,
        )
        return (new_high, total, numerator)

    highest, total, numerator = lax.fori_loop(0, count, step, start_state)
    attended = (numerator / total[..., None]).transpose(1, 0, 2).reshape(query_rows, local_width)
    attended = attended.astype(jnp.bfloat16)
    columns = jnp.dot(
        lax.all_gather(attended, "ulysses", axis=1, tiled=True),
        out_weight,
        preferred_element_type=jnp.float32,
    )
    branch = lax.all_to_all(
        columns.astype(jnp.bfloat16), "ulysses", split_axis=0, concat_axis=1, tiled=True
    ).astype(columns.dtype)
    return (wide + mod_gate * branch).astype(jnp.bfloat16)


def solution(mesh):
    in_specs = (
        P(("blk", "ulysses"), None),
        P(),
        P(),
        P(),
        P(None, None, "ulysses"),
        P(),
        P(),
        P(None, "ulysses"),
    )
    out_specs = P(("blk", "ulysses"), None)
    blocks, group = mesh.shape["blk"], mesh.shape["ulysses"]

    def body(*args):
        tokens, head, width = args[0], args[5].shape[0], args[4].shape[2]
        pairs_split = width % (2 * head) == 0 and tokens.shape[0] % (16 * PARTS) == 0
        if blocks == 8 and pairs_split:
            return paired(blocks, group, *args)
        return local(*args)

    return jax.shard_map(body, mesh=mesh, in_specs=in_specs, out_specs=out_specs, check_vma=False)
```
